32 devices in a mesh: data: 1 (over z), expert: 32 (over y, x, core).
Axes of the slice: x: 4, y: 4, z: 1, core: 2. Of those that a mesh axis runs over, the one named last changes fastest.
The devices are a block of a 4x4x8 slice.
Arguments:
- x: bfloat16 [24576, 2048], P(('data', 'expert'))
- idx: int32 [24576, 7], P(('data', 'expert'))
- g: float32 [24576, 7], P(('data', 'expert'))
- hot_tok: int32 [12288], P(('data', 'expert'))
- hot_g: float32 [12288], P(('data', 'expert'))
- ln1: float32 [2048], replicated
- wq: bfloat16 [2048, 16, 128], replicated
- wk: bfloat16 [2048, 16, 128], replicated
- wv: bfloat16 [2048, 16, 128], replicated
- wo: bfloat16 [16, 128, 2048], replicated
- ln2: float32 [2048], replicated
- w1: bfloat16 [64, 2048, 1024], P('expert')
- w3: bfloat16 [64, 2048, 1024], P('expert')
- w2: bfloat16 [64, 1024, 2048], P('expert')
Outputs:
- output: bfloat16 [24576, 2048], P(('data', 'expert'))
All inputs are finite; a program needn't handle non-finite values.
Results may differ from the reference program's by a relative error of at most 0.0105547.
Values are sent between devices in bfloat16 or wider.
A program may use at most 768 MiB of HBM per device.

```python
import jax
import jax.numpy as jnp
from jax import lax

D = 2048
FF = 1024
EXPERTS = 64
TOP = 8
HEADS = 16
HEAD = 128
TOKENS = 768
NDEV = 32
HOT = 384
HOT_ID = 1

KC = TOP - 1
C0 = (TOKENS * KC + EXPERTS - 2) // (EXPERTS - 1)
CAP = 8 * ((3 * C0 + 15) // 16)
EPS = 1e-6
ROPE_BASE = 10000.0


def _routing(key):
    k1, k2, k3, k4, k5 = jax.random.split(key, 5)
    d1, d2, d3 = jax.random.split(jax.random.fold_in(key, 7), 3)
    used = (EXPERTS - 1) - (EXPERTS - 1) // 3
    rank = jax.random.permutation(d1, TOKENS)
    c = (rank[:, None] * KC + jnp.arange(KC)[None, :]) % used
    cold = jax.random.permutation(d2, EXPERTS - 1)[c]
    idx = (cold + (cold >= HOT_ID)).astype(jnp.int32)
    start = jax.random.randint(d3, (), 0, TOKENS)
    hot_tok = ((start + jnp.arange(HOT)) % TOKENS).astype(jnp.int32)
    is_hot = jnp.zeros((TOKENS,), jnp.float32).at[hot_tok].set(1.0)
    lc = jax.random.normal(k4, (TOKENS, KC), jnp.float32)
    lh = jax.random.normal(k5, (TOKENS,), jnp.float32) + 1.0
    m = jnp.maximum(jnp.max(lc, axis=1), lh)
    ec = jnp.exp(lc - m[:, None])
    eh = jnp.exp(lh - m) * is_hot
    den = jnp.sum(ec, axis=1) + eh
    return idx, ec / den[:, None], hot_tok, (eh / den)[hot_tok]


def _normal(key, shape, fan_in):
    return (jax.random.normal(key, shape, jnp.float32) * fan_in ** -0.5).astype(jnp.bfloat16)


def _expert_weights(key, shape, fan_in):
    return lax.map(lambda k: _normal(k, shape, fan_in), jax.random.split(key, EXPERTS))


def setup_inputs(seed: int = 0, part: int = 0) -> dict:
    key = jax.random.PRNGKey(seed)
    ks = jax.random.split(key, 9)
    kx, kr = jax.random.split(jax.random.fold_in(key, part))
    x = jax.random.normal(kx, (NDEV * TOKENS, D), jnp.float32).astype(jnp.bfloat16)
    idx, g, hot_tok, hot_g = jax.vmap(_routing)(jax.random.split(kr, NDEV))
    return {
        'x': x,
        'idx': idx.reshape(NDEV * TOKENS, KC),
        'g': g.reshape(NDEV * TOKENS, KC),
        'hot_tok': hot_tok.reshape(NDEV * HOT),
        'hot_g': hot_g.reshape(NDEV * HOT),
        'ln1': jax.random.uniform(ks[0], (D,), jnp.float32, 0.5, 1.5),
        'wq': _normal(ks[1], (D, HEADS, HEAD), D),
        'wk': _normal(ks[2], (D, HEADS, HEAD), D),
        'wv': _normal(ks[3], (D, HEADS, HEAD), D),
        'wo': _normal(ks[4], (HEADS, HEAD, D), HEADS * HEAD),
        'ln2': jax.random.uniform(ks[5], (D,), jnp.float32, 0.5, 1.5),
        'w1': _expert_weights(ks[6], (D, FF), D),
        'w3': _expert_weights(ks[7], (D, FF), D),
        'w2': _expert_weights(ks[8], (FF, D), FF),
    }


def _rms(v, w):
    v = v.astype(jnp.float32)
    return (v * lax.rsqrt(jnp.mean(v * v, axis=-1, keepdims=True) + EPS) * w).astype(jnp.bfloat16)


def _rope(t):
    half = HEAD // 2
    freq = ROPE_BASE ** (-jnp.arange(half, dtype=jnp.float32) / half)
    ang = jnp.arange(TOKENS, dtype=jnp.float32)[:, None] * freq[None, :]
    cos = jnp.cos(ang)[:, None, :]
    sin = jnp.sin(ang)[:, None, :]
    t1, t2 = t[..., :half], t[..., half:]
    return jnp.concatenate([t1 * cos - t2 * sin, t2 * cos + t1 * sin], axis=-1)


def _attention(x, ln1, wq, wk, wv, wo):
    a = _rms(x, ln1).astype(jnp.float32)
    q = _rope(jnp.einsum('td,dhk->thk', a, wq.astype(jnp.float32))).astype(jnp.bfloat16)
    k = _rope(jnp.einsum('td,dhk->thk', a, wk.astype(jnp.float32))).astype(jnp.bfloat16)
    v = jnp.einsum('td,dhk->thk', a, wv.astype(jnp.float32)).astype(jnp.bfloat16)
    mask = jnp.tril(jnp.ones((TOKENS, TOKENS), bool))

    def head(qkv):
        qh, kh, vh = qkv
        s = jnp.dot(qh, kh.T, preferred_element_type=jnp.float32) * HEAD ** -0.5
        p = jax.nn.softmax(jnp.where(mask, s, -jnp.inf), axis=-1).astype(jnp.bfloat16)
        return jnp.dot(p, vh, preferred_element_type=jnp.float32).astype(jnp.bfloat16)

    o = lax.map(head, (q.transpose(1, 0, 2), k.transpose(1, 0, 2), v.transpose(1, 0, 2)))
    out = jnp.einsum('htk,hkd->td', o.astype(jnp.float32), wo.astype(jnp.float32))
    return (x.astype(jnp.float32) + out).astype(jnp.bfloat16)


def _ffn(a, w1, w3, w2):
    h1 = jnp.dot(a, w1, preferred_element_type=jnp.float32)
    h3 = jnp.dot(a, w3, preferred_element_type=jnp.float32)
    z = (jax.nn.silu(h1) * h3).astype(jnp.bfloat16)
    return jnp.dot(z, w2, preferred_element_type=jnp.float32).astype(jnp.bfloat16)


def reference(x, idx, g, hot_tok, hot_g, ln1, wq, wk, wv, wo, ln2, w1, w3, w2):
    h = lax.map(lambda s: _attention(s, ln1, wq, wk, wv, wo), x.reshape(NDEV, TOKENS, D))
    u = _rms(h.reshape(NDEV * TOKENS, D), ln2)
    e = idx.reshape(-1)
    r_all = e.shape[0]
    order = jnp.argsort(e, stable=True)
    counts = jnp.zeros((EXPERTS,), jnp.int32).at[e].add(1)
    starts = jnp.cumsum(counts) - counts
    gf = g.reshape(-1)
    rows = jnp.arange(NDEV * CAP)

    def body(y, ex):
        r = order[jnp.minimum(starts[ex] + rows, r_all - 1)]
        tok = r // KC
        out = _ffn(u[tok], w1[ex], w3[ex], w2[ex]).astype(jnp.float32)
        w = jnp.where(rows < counts[ex], gf[r], 0.0)
        return y.at[tok].add(w[:, None] * out), None

    y, _ = lax.scan(body, jnp.zeros((NDEV * TOKENS, D), jnp.float32), jnp.arange(EXPERTS))
    ht = hot_tok + jnp.repeat(jnp.arange(NDEV, dtype=jnp.int32) * TOKENS, HOT)
    ho = _ffn(u[ht], w1[HOT_ID], w3[HOT_ID], w2[HOT_ID]).astype(jnp.float32)
    y = y.at[ht].add(hot_g[:, None] * ho)
    return y.astype(jnp.bfloat16)
```

```python
import jax
import jax.numpy as jnp
from jax import lax
from jax.sharding import PartitionSpec as P

EPS = 1e-6
ROPE_BASE = 10000.0
HOT_ID = 1
CHUNKS = 2
F32 = jnp.float32
BF16 = jnp.bfloat16


def _rms(v, w):
    v = v.astype(F32)
    return (v * lax.rsqrt(jnp.mean(v * v, axis=-1, keepdims=True) + EPS) * w).astype(BF16)


def _rope(t, start):
    n_tok, _, dh = t.shape
    half = dh // 2
    freq = ROPE_BASE ** (-jnp.arange(half, dtype=F32) / half)
    ang = (start + jnp.arange(n_tok, dtype=F32))[:, None] * freq[None, :]
    cos = jnp.cos(ang)[:, None, :]
    sin = jnp.sin(ang)[:, None, :]
    t1, t2 = t[..., :half], t[..., half:]
    return jnp.concatenate([t1 * cos - t2 * sin, t2 * cos + t1 * sin], axis=-1)


def _attention_chunks(x, ln1, wq, wk, wv, wo, chunks):
    n_tok = x.shape[0]
    dh = wq.shape[2]
    step = n_tok // chunks
    ks, vs = [], []
    before = None
    for c in range(chunks):
        lo = c * step
        xc = x[lo:lo + step]
        if before is not None:
            xc, _ = lax.optimization_barrier((xc, before))
        a = _rms(xc, ln1)
        q = _rope(jnp.einsum('td,dhk->thk', a, wq, preferred_element_type=F32), lo).astype(BF16)
        ks.append(_rope(jnp.einsum('td,dhk->thk', a, wk, preferred_element_type=F32), lo).astype(BF16))
        vs.append(jnp.einsum('td,dhk->thk', a, wv, preferred_element_type=F32).astype(BF16))
        k = jnp.concatenate(ks, axis=0)
        v = jnp.concatenate(vs, axis=0)
        s = jnp.einsum('qhk,shk->hqs', q, k, preferred_element_type=F32) * dh ** -0.5
        mask = (lo + jnp.arange(step))[:, None] >= jnp.arange(lo + step)[None, :]
        p = jax.nn.softmax(jnp.where(mask[None], s, -jnp.inf), axis=-1).astype(BF16)
        o = jnp.einsum('hqs,shk->qhk', p, v, preferred_element_type=F32).astype(BF16)
        out = jnp.einsum('qhk,hkd->qd', o, wo, preferred_element_type=F32)
        before = yield (xc.astype(F32) + out).astype(BF16)


def _capacity(t, kc, n_exp):
    c0 = (t * kc + n_exp - 2) // (n_exp - 1)
    return 8 * ((3 * c0 + 15) // 16)


def _ffn(a, w1, w3, w2):
    h1 = jnp.dot(a, w1, preferred_element_type=F32)
    h3 = jnp.dot(a, w3, preferred_element_type=F32)
    z = (jax.nn.silu(h1) * h3).astype(BF16)
    return jnp.dot(z, w2, preferred_element_type=F32).astype(BF16)


def _parts(g):
    hi = lax.reduce_precision(g, 8, 7)
    mid = lax.reduce_precision(g - hi, 8, 7)
    low = g - hi - mid
    return [v.astype(BF16) for v in (hi, mid, low)]


def _gated(g_parts, hit, rows):
    lhs = jnp.concatenate([jnp.where(hit, v, jnp.zeros((), BF16)) for v in g_parts], axis=0)
    out = jnp.dot(lhs, rows, preferred_element_type=F32)
    return jnp.sum(out.reshape(len(g_parts), -1, out.shape[-1]), axis=0)


def solution(mesh):
    n = mesh.shape['expert']

    def local(x, idx, g, hot_tok, hot_g, ln1, wq, wk, wv, wo, ln2, w1, w3, w2):
        T, D = x.shape
        KC = idx.shape[1]
        el = w1.shape[0]
        E = el * n
        C = _capacity(T, KC, E)
        owner = HOT_ID // el
        lh = HOT_ID % el
        me = lax.axis_index('expert')

        own = me == owner
        hw = [lax.psum(jnp.where(own, w[lh], jnp.zeros((), BF16)), 'expert') for w in (w1, w3, w2)]

        same = idx[:, :, None] == jnp.arange(E, dtype=jnp.int32)
        has = jnp.any(same, axis=1)
        gate = jnp.sum(jnp.where(same, g[:, :, None], 0.0), axis=1)
        tri = jnp.tril(jnp.ones((T, T), BF16))
        upto = jnp.dot(tri, has.astype(BF16), preferred_element_type=F32)
        place = jnp.where(has, upto.astype(jnp.int32) - 1, -1)
        theirs = lax.all_to_all(place.T, 'expert', 0, 0, tiled=True).reshape(n, el, T)

        step = T // CHUNKS
        us = []
        xin = [None] * el
        slot = jnp.arange(C, dtype=jnp.int32)
        chunks = _attention_chunks(x, ln1, wq, wk, wv, wo, CHUNKS)
        u = None
        for c in range(CHUNKS):
            u = _rms(chunks.send(u), ln2)
            if c == 0:
                u, *hw = lax.optimization_barrier((u, *hw))
            us.append(u)
            every = lax.all_gather(u, 'expert')
            for l in range(el):
                pick = (theirs[:, l, None, c * step:(c + 1) * step] == slot[:, None]).astype(BF16)
                part = jnp.einsum('srt,std->srd', pick, every, preferred_element_type=F32).astype(BF16)
                xin[l] = part if xin[l] is None else xin[l] + part
        u = jnp.concatenate(us, axis=0)

        y = jnp.zeros((T, D), F32)
        hot_hit = hot_tok[:, None] == jnp.arange(T, dtype=jnp.int32)
        hot_rows = jnp.dot(hot_hit.astype(BF16), u, preferred_element_type=F32).astype(BF16)
        hot_out = _ffn(hot_rows, *hw)
        y = y + _gated([v[None, :] for v in _parts(hot_g)], hot_hit.T, hot_out)

        g_parts = _parts(gate)
        for l in range(el):
            out = _ffn(xin[l].reshape(n * C, D), w1[l], w3[l], w2[l])
            back = lax.all_to_all(out, 'expert', 0, 0, tiled=True)
            hit = (place.reshape(T, n, el)[:, :, l, None] == slot).reshape(T, n * C)
            gl = [jnp.broadcast_to(v.reshape(T, n, el)[:, :, l, None], (T, n, C)).reshape(T, n * C)
                  for v in g_parts]
            y = y + _gated(gl, hit, back)
        return y.astype(BF16)

    tk = ('data', 'expert')
    rep3 = P(None, None, None)
    exp3 = P('expert', None, None)
    return jax.shard_map(
        local, mesh=mesh,
        in_specs=(P(tk, None), P(tk, None), P(tk, None), P(tk), P(tk), P(None),
                  rep3, rep3, rep3, rep3, P(None), exp3, exp3, exp3),
        out_specs=P(tk, None), check_vma=False)
```

```python
import functools
import math

import jax
import jax.numpy as jnp
from jax import lax
from jax.experimental import pallas as pl
from jax.experimental.pallas import tpu as pltpu
from jax.sharding import PartitionSpec as P

EPS = 1e-6
ROPE_BASE = 10000.0
HOT_ID = 1
CHUNKS = 1
F32 = jnp.float32
BF16 = jnp.bfloat16


def _rms(v, w):
    v = v.astype(F32)
    return (v * lax.rsqrt(jnp.mean(v * v, axis=-1, keepdims=True) + EPS) * w).astype(BF16)


def _rope(t, start):
    n_tok, _, dh = t.shape
    half = dh // 2
    freq = ROPE_BASE ** (-jnp.arange(half, dtype=F32) / half)
    ang = (start + jnp.arange(n_tok, dtype=F32))[:, None] * freq[None, :]
    cos = jnp.cos(ang)[:, None, :]
    sin = jnp.sin(ang)[:, None, :]
    t1, t2 = t[..., :half], t[..., half:]
    return jnp.concatenate([t1 * cos - t2 * sin, t2 * cos + t1 * sin], axis=-1)


def _attention_chunks(x, ln1, wq, wk, wv, wo, chunks):
    n_tok = x.shape[0]
    dh = wq.shape[2]
    step = n_tok // chunks
    ks, vs = [], []
    before = None
    for c in range(chunks):
        lo = c * step
        xc = x[lo:lo + step]
        if before is not None:
            xc, _ = lax.optimization_barrier((xc, before))
        a = _rms(xc, ln1)
        q = _rope(jnp.einsum('td,dhk->thk', a, wq, preferred_element_type=F32), lo).astype(BF16)
        ks.append(_rope(jnp.einsum('td,dhk->thk', a, wk, preferred_element_type=F32), lo).astype(BF16))
        vs.append(jnp.einsum('td,dhk->thk', a, wv, preferred_element_type=F32).astype(BF16))
        k = jnp.concatenate(ks, axis=0)
        v = jnp.concatenate(vs, axis=0)
        s = jnp.einsum('qhk,shk->hqs', q, k, preferred_element_type=F32) * dh ** -0.5
        mask = (lo + jnp.arange(step))[:, None] >= jnp.arange(lo + step)[None, :]
        p = jax.nn.softmax(jnp.where(mask[None], s, -jnp.inf), axis=-1).astype(BF16)
        o = jnp.einsum('hqs,shk->qhk', p, v, preferred_element_type=F32).astype(BF16)
        out = jnp.einsum('qhk,hkd->qd', o, wo, preferred_element_type=F32)
        before = yield (xc.astype(F32) + out).astype(BF16)


def _capacity(t, kc, n_exp):
    c0 = (t * kc + n_exp - 2) // (n_exp - 1)
    return 8 * ((3 * c0 + 15) // 16)


def _ffn(a, w1, w3, w2):
    h1 = jnp.dot(a, w1, preferred_element_type=F32)
    h3 = jnp.dot(a, w3, preferred_element_type=F32)
    z = (jax.nn.silu(h1) * h3).astype(BF16)
    return jnp.dot(z, w2, preferred_element_type=F32).astype(BF16)


def _parts(g):
    hi = lax.reduce_precision(g, 8, 7)
    mid = lax.reduce_precision(g - hi, 8, 7)
    low = g - hi - mid
    return [v.astype(BF16) for v in (hi, mid, low)]


def _gated(g_parts, hit, rows):
    lhs = jnp.concatenate([jnp.where(hit, v, jnp.zeros((), BF16)) for v in g_parts], axis=0)
    out = jnp.dot(lhs, rows, preferred_element_type=F32)
    return jnp.sum(out.reshape(len(g_parts), -1, out.shape[-1]), axis=0)


def _up(v, m):
    return (v + m - 1) // m * m


def _exchange(n, axis, theirs, u_all, w1, w3, w2, gates, y0,
              y_out, recv, stage,
              ubuf, v1, v3, v2, xin, z, out, y, gbuf, rbuf,
              u_sem, w_sem, o_sem, y_sem, g_sem, r_sem, send_sem, recv_sem):
    T, D = y.shape
    el, CP = 2, xin.shape[1] // 4
    C2 = recv.shape[1]
    C = C2 // 2
    FF = z.shape[2]
    side = math.isqrt(n // 2)
    FT, NT = min(256, FF), min(256, D)
    me = lax.axis_index(axis)
    core, chip = lax.rem(me, 2), lax.div(me, 2)
    cx, cy = lax.rem(chip, side), lax.div(chip, side)

    def chip_at(o, sign):
        dx = lax.rem(o + 1, side)
        dy = lax.rem(o + 1 + lax.div(o, side), side)
        px = lax.rem(cx + sign * dx + side, side)
        py = lax.rem(cy + sign * dy + side, side)
        return py * side + px

    def dest(k):
        return chip_at(lax.div(k, 2), 1) * 2 + lax.rem(k, 2)

    def u_copy(k, slot):
        return pltpu.make_async_copy(u_all.at[dest(k)], ubuf.at[slot], u_sem.at[slot])

    def g_copy(c, slot):
        return pltpu.make_async_copy(gates.at[chip_at(c, -1)], gbuf.at[slot], g_sem.at[slot])

    def send(d):
        return pltpu.make_async_remote_copy(
            src_ref=stage.at[d], dst_ref=recv.at[me],
            send_sem=send_sem.at[d], recv_sem=recv_sem.at[me],
            device_id={axis: d}, device_id_type=pl.DeviceIdType.MESH)

    weights = [pltpu.make_async_copy(a, b, w_sem.at[i])
               for i, (a, b) in enumerate(((w1, v1), (w3, v3), (w2, v2)))]
    u_copy(0, 0).start()
    u_copy(1, 1).start()
    for cp in weights:
        cp.start()
    y_copy = pltpu.make_async_copy(y0, y, y_sem.at[0])
    y_copy.start()
    g_copy(0, 0).start()

    barrier = pltpu.get_barrier_semaphore()

    @pl.loop(1, n)
    def _(k):
        pl.semaphore_signal(barrier, inc=1, device_id={axis: lax.rem(me + k, n)},
                            device_id_type=pl.DeviceIdType.MESH)

    pl.semaphore_wait(barrier, n - 1)
    rbuf[:, 2 * C2:, :] = jnp.zeros((2, rbuf.shape[1] - 2 * C2, D), BF16)

    @pl.loop(0, n // 4)
    def _(b):
        for j in range(4):
            k = b * 4 + j
            slot = j % 2
            u_copy(k, slot).wait()
            where = theirs[dest(k)]
            rows = lax.broadcasted_iota(jnp.int32, (CP, T), 0)
            pick = [(where[l:l + 1, :] == rows).astype(F32).astype(BF16) for l in range(el)]

            @pl.loop(0, D // NT)
            def _(i):
                cols = pl.ds(pl.multiple_of(i * NT, NT), NT)
                for l in range(el):
                    xin[l, j * CP:(j + 1) * CP, cols] = jnp.dot(
                        pick[l], ubuf[slot, :, cols], preferred_element_type=F32).astype(BF16)

            @pl.when(k + 2 < n)
            def _():
                u_copy(k + 2, slot).start()

        @pl.when(b == 0)
        def _():
            for cp in weights:
                cp.wait()

        for l in range(el):
            @pl.loop(0, FF // FT)
            def _(i):
                cols = pl.ds(pl.multiple_of(i * FT, FT), FT)
                h1 = jnp.dot(xin[l], v1[l, :, cols], preferred_element_type=F32)
                h3 = jnp.dot(xin[l], v3[l, :, cols], preferred_element_type=F32)
                z[l, :, cols] = (h1 * jax.nn.sigmoid(h1) * h3).astype(BF16)

        @pl.loop(0, D // NT)
        def _(i):
            cols = pl.ds(pl.multiple_of(i * NT, NT), NT)
            o0 = jnp.dot(z[0], v2[0, :, cols], preferred_element_type=F32)
            o1 = jnp.dot(z[1], v2[1, :, cols], preferred_element_type=F32)
            for j in range(4):
                both = jnp.concatenate([o0[j * CP:j * CP + C], o1[j * CP:j * CP + C]], axis=0)
                out[j, :, cols] = both.astype(BF16)

        for j in range(4):
            d = dest(b * 4 + j)

            @pl.when(d != me)
            def _():
                pltpu.make_async_copy(out.at[j], stage.at[d], o_sem.at[j]).start()

            @pl.when(d == me)
            def _():
                pltpu.make_async_copy(out.at[j], recv.at[me], o_sem.at[j]).start()

        for j in range(4):
            d = dest(b * 4 + j)

            @pl.when(d != me)
            def _():
                pltpu.make_async_copy(out.at[j], stage.at[d], o_sem.at[j]).wait()
                send(d).start()

            @pl.when(d == me)
            def _():
                pltpu.make_async_copy(out.at[j], recv.at[me], o_sem.at[j]).wait()

    y_copy.wait()

    def from_chip(c, slot):
        e = chip_at(c, -1) * 2
        return e, [pltpu.make_async_copy(recv.at[e + i], rbuf.at[slot, i * C2:(i + 1) * C2], r_sem.at[slot, i])
                   for i in range(2)]

    @pl.loop(0, n // 4)
    def _(cc):
        for slot in range(2):
            c = cc * 2 + slot
            e, copies = from_chip(c, slot)
            for i in range(2):
                @pl.when(e + i != me)
                def _():
                    pltpu.make_async_remote_copy(
                        src_ref=stage.at[e + i], dst_ref=recv.at[e + i],
                        send_sem=send_sem.at[e + i], recv_sem=recv_sem.at[e + i],
                        device_id={axis: me}, device_id_type=pl.DeviceIdType.MESH).wait_recv()
                copies[i].start()

            @pl.when(c + 1 < n // 2)
            def _():
                g_copy(c + 1, 1 - slot).start()

            g_copy(c, slot).wait()
            for cp in copies:
                cp.wait()

            @pl.loop(0, D // NT)
            def _(i):
                cols = pl.ds(pl.multiple_of(i * NT, NT), NT)
                acc = y[:, cols]
                for p in range(3):
                    acc = acc + jnp.dot(gbuf[slot, p], rbuf[slot, :, cols], preferred_element_type=F32)
                y[:, cols] = acc

    @pl.loop(0, D // NT)
    def _(i):
        cols = pl.ds(pl.multiple_of(i * NT, NT), NT)
        ubuf[0, :, cols] = y[:, cols].astype(BF16)

    done = pltpu.make_async_copy(ubuf.at[0], y_out, y_sem.at[0])
    done.start()
    done.wait()

    @pl.loop(0, n)
    def _(d):
        @pl.when(d != me)
        def _():
            send(d).wait_send()


def _run_exchange(n, axis, C, theirs, u_all, w1, w3, w2, gates, y0):
    T, D = y0.shape
    el, _, FF = w1.shape
    C2, CP = 2 * C, _up(C, 16)
    KP = gates.shape[-1]
    any_spec = pl.BlockSpec(memory_space=pl.ANY)
    dma = pltpu.SemaphoreType.DMA
    rows = n * 2 * C
    return pl.pallas_call(
        functools.partial(_exchange, n, axis),
        out_shape=(jax.ShapeDtypeStruct((T, D), BF16),
                   jax.ShapeDtypeStruct((n, C2, D), BF16),
                   jax.ShapeDtypeStruct((n, C2, D), BF16)),
        in_specs=[pl.BlockSpec(memory_space=pltpu.VMEM)] + [any_spec] * 6,
        out_specs=(any_spec,) * 3,
        scratch_shapes=[
            pltpu.VMEM((2, T, D), BF16),
            pltpu.VMEM((el, D, FF), BF16),
            pltpu.VMEM((el, D, FF), BF16),
            pltpu.VMEM((el, FF, D), BF16),
            pltpu.VMEM((el, 4 * CP, D), BF16),
            pltpu.VMEM((el, 4 * CP, FF), BF16),
            pltpu.VMEM((4, C2, D), BF16),
            pltpu.VMEM((T, D), F32),
            pltpu.VMEM((2, 3, T, KP), BF16),
            pltpu.VMEM((2, KP, D), BF16),
            dma((2,)), dma((3,)), dma((4,)), dma((1,)), dma((2,)), dma((2, 2)), dma((n,)), dma((n,)),
        ],
        compiler_params=pltpu.CompilerParams(
            collective_id=0, has_side_effects=True, vmem_limit_bytes=66 * 1000 * 1000),
        cost_estimate=pl.CostEstimate(
            flops=rows * 6 * D * FF + rows * 8 * T * D, bytes_accessed=rows * D * 8, transcendentals=rows * FF),
        name='exchange',
    )(theirs, u_all, w1, w3, w2, gates, y0)[0]


def solution(mesh):
    n = mesh.shape['expert']

    def local(x, idx, g, hot_tok, hot_g, ln1, wq, wk, wv, wo, ln2, w1, w3, w2):
        T, D = x.shape
        KC = idx.shape[1]
        el = w1.shape[0]
        E = el * n
        C = _capacity(T, KC, E)
        owner = HOT_ID // el
        lh = HOT_ID % el
        me = lax.axis_index('expert')

        own = me == owner
        hw = [lax.psum(jnp.where(own, w[lh], jnp.zeros((), BF16)), 'expert') for w in (w1, w3, w2)]

        same = idx[:, :, None] == jnp.arange(E, dtype=jnp.int32)
        has = jnp.any(same, axis=1)
        gate = jnp.sum(jnp.where(same, g[:, :, None], 0.0), axis=1)
        tri = jnp.tril(jnp.ones((T, T), BF16))
        upto = jnp.dot(tri, has.astype(BF16), preferred_element_type=F32)
        place = jnp.where(has, upto.astype(jnp.int32) - 1, -1)
        theirs = lax.all_to_all(place.T, 'expert', 0, 0, tiled=True).reshape(n, el, T)
        theirs = jnp.pad(theirs, ((0, 0), (0, 8 - el), (0, 0)), constant_values=-1)

        per = 2 * el
        col = jnp.arange(_up(per * C, 128), dtype=jnp.int32)
        key = jnp.where(has, place + (jnp.arange(E, dtype=jnp.int32) % per) * C, -1)
        key = key.reshape(T, E // per, per).transpose(1, 0, 2)
        parts = jnp.stack(_parts(gate)).reshape(3, T, E // per, per).transpose(2, 0, 1, 3)
        gates = jnp.zeros((), BF16)
        for k in range(per):
            hit = key[:, None, :, k, None] == col
            gates = jnp.where(hit, parts[:, :, :, k, None], gates)

        chunks = _attention_chunks(x, ln1, wq, wk, wv, wo, CHUNKS)
        u = _rms(chunks.send(None), ln2)
        u, *hw = lax.optimization_barrier((u, *hw))
        u_all = lax.all_gather(u, 'expert')

        hot_hit = hot_tok[:, None] == jnp.arange(T, dtype=jnp.int32)
        hot_rows = jnp.dot(hot_hit.astype(BF16), u, preferred_element_type=F32).astype(BF16)
        hot_out = _ffn(hot_rows, *hw)
        y0 = _gated([v[None, :] for v in _parts(hot_g)], hot_hit.T, hot_out)
        return _run_exchange(n, 'expert', C, theirs, u_all, w1, w3, w2, gates, y0)

    tk = ('data', 'expert')
    rep3 = P(None, None, None)
    exp3 = P('expert', None, None)
    return jax.shard_map(
        local, mesh=mesh,
        in_specs=(P(tk, None), P(tk, None), P(tk, None), P(tk), P(tk), P(None),
                  rep3, rep3, rep3, rep3, P(None), exp3, exp3, exp3),
        out_specs=P(tk, None), check_vma=False)
```

```python
import functools
import math

import jax
import jax.numpy as jnp
from jax import lax
from jax.experimental import pallas as pl
from jax.experimental.pallas import tpu as pltpu
from jax.sharding import PartitionSpec as P

EPS = 1e-6
ROPE_BASE = 10000.0
HOT_ID = 1
CHUNKS = 1
F32 = jnp.float32
BF16 = jnp.bfloat16


def _rms(v, w):
    v = v.astype(F32)
    return (v * lax.rsqrt(jnp.mean(v * v, axis=-1, keepdims=True) + EPS) * w).astype(BF16)


def _rope(t, start):
    n_tok, _, dh = t.shape
    half = dh // 2
    freq = ROPE_BASE ** (-jnp.arange(half, dtype=F32) / half)
    ang = (start + jnp.arange(n_tok, dtype=F32))[:, None] * freq[None, :]
    cos = jnp.cos(ang)[:, None, :]
    sin = jnp.sin(ang)[:, None, :]
    t1, t2 = t[..., :half], t[..., half:]
    return jnp.concatenate([t1 * cos - t2 * sin, t2 * cos + t1 * sin], axis=-1)


def _attention_chunks(x, ln1, wq, wk, wv, wo, chunks):
    n_tok = x.shape[0]
    dh = wq.shape[2]
    step = n_tok // chunks
    ks, vs = [], []
    before = None
    for c in range(chunks):
        lo = c * step
        xc = x[lo:lo + step]
        if before is not None:
            xc, _ = lax.optimization_barrier((xc, before))
        a = _rms(xc, ln1)
        q = _rope(jnp.einsum('td,dhk->thk', a, wq, preferred_element_type=F32), lo).astype(BF16)
        ks.append(_rope(jnp.einsum('td,dhk->thk', a, wk, preferred_element_type=F32), lo).astype(BF16))
        vs.append(jnp.einsum('td,dhk->thk', a, wv, preferred_element_type=F32).astype(BF16))
        k = jnp.concatenate(ks, axis=0)
        v = jnp.concatenate(vs, axis=0)
        s = jnp.einsum('qhk,shk->hqs', q, k, preferred_element_type=F32) * dh ** -0.5
        mask = (lo + jnp.arange(step))[:, None] >= jnp.arange(lo + step)[None, :]
        p = jax.nn.softmax(jnp.where(mask[None], s, -jnp.inf), axis=-1).astype(BF16)
        o = jnp.einsum('hqs,shk->qhk', p, v, preferred_element_type=F32).astype(BF16)
        out = jnp.einsum('qhk,hkd->qd', o, wo, preferred_element_type=F32)
        before = yield (xc.astype(F32) + out).astype(BF16)


def _capacity(t, kc, n_exp):
    c0 = (t * kc + n_exp - 2) // (n_exp - 1)
    return 8 * ((3 * c0 + 15) // 16)


def _ffn(a, w1, w3, w2):
    h1 = jnp.dot(a, w1, preferred_element_type=F32)
    h3 = jnp.dot(a, w3, preferred_element_type=F32)
    z = (jax.nn.silu(h1) * h3).astype(BF16)
    return jnp.dot(z, w2, preferred_element_type=F32).astype(BF16)


def _parts(g):
    hi = lax.reduce_precision(g, 8, 7)
    mid = lax.reduce_precision(g - hi, 8, 7)
    low = g - hi - mid
    return [v.astype(BF16) for v in (hi, mid, low)]


def _gated(g_parts, hit, rows):
    lhs = jnp.concatenate([jnp.where(hit, v, jnp.zeros((), BF16)) for v in g_parts], axis=0)
    out = jnp.dot(lhs, rows, preferred_element_type=F32)
    return jnp.sum(out.reshape(len(g_parts), -1, out.shape[-1]), axis=0)


def _up(v, m):
    return (v + m - 1) // m * m


ORDER4 = ((0, 1), (2, 0), (1, 3), (0, 2), (0, 0), (3, 0), (1, 1), (2, 1),
          (0, 3), (3, 3), (3, 1), (1, 0), (2, 3), (3, 2), (2, 2), (1, 2))


def _side(n):
    return math.isqrt(n // 2)


def _offset(side, o):
    order = ORDER4 if side == 4 else tuple((i % side, i // side) for i in range(side * side))

    def digit(vals):
        lo, hi = (sum(v * 4 ** i for i, v in enumerate(vals[h * 8:h * 8 + 8])) for h in range(2))
        q = lax.rem(o, 8)
        power = ((1 + 3 * lax.rem(q, 2)) * (1 + 15 * lax.rem(lax.div(q, 2), 2)) * (1 + 255 * lax.div(q, 4)))
        return lax.rem(lax.div(lo + lax.div(o, 8) * (hi - lo), power), 4)

    return digit([v[0] for v in order]), digit([v[1] for v in order])


def _peer(n, me, k, sending):
    side = _side(n)
    core, chip = lax.rem(me, 2), lax.div(me, 2)
    other = lax.rem(k, 2)
    dx, dy = _offset(side, lax.div(k, 2))
    their = lax.rem(core + other, 2)
    sign = 1 - 2 * core if sending else 2 * their - 1
    px = lax.rem(lax.rem(chip, side) + sign * dx + side, side)
    py = lax.rem(lax.div(chip, side) + sign * dy + side, side)
    return (py * side + px) * 2 + their


def _exchange(n, axis, theirs, u_all, w1, w3, w2, marks, y0,
              y_out, recv, stage,
              ubuf, v1, v3, v2, xin, z, out, y, mbuf, sel, rbuf,
              u_sem, w_sem, o_sem, y_sem, m_sem, r_sem, send_sem, recv_sem):
    T, D = y.shape
    el, CP = 2, xin.shape[1] // 4
    C2 = recv.shape[1]
    C = C2 // 2
    FF = z.shape[2]
    KW = sel.shape[2]
    FT, NT = min(256, FF), min(256, D)
    me = lax.axis_index(axis)

    def dest(k):
        return _peer(n, me, k, True)

    def u_copy(k, slot):
        return pltpu.make_async_copy(u_all.at[dest(k)], ubuf.at[slot], u_sem.at[slot])

    def m_copy(c, slot):
        return pltpu.make_async_copy(marks.at[c], mbuf.at[slot], m_sem.at[slot])

    def send(d):
        return pltpu.make_async_remote_copy(
            src_ref=stage.at[d], dst_ref=recv.at[me],
            send_sem=send_sem.at[d], recv_sem=recv_sem.at[me],
            device_id={axis: d}, device_id_type=pl.DeviceIdType.MESH)

    weights = [pltpu.make_async_copy(a, b, w_sem.at[i])
               for i, (a, b) in enumerate(((w1, v1), (w3, v3), (w2, v2)))]
    u_copy(0, 0).start()
    u_copy(1, 1).start()
    for cp in weights:
        cp.start()
    y_copy = pltpu.make_async_copy(y0, y, y_sem.at[0])
    y_copy.start()
    m_copy(0, 0).start()

    barrier = pltpu.get_barrier_semaphore()

    @pl.loop(1, n)
    def _(k):
        pl.semaphore_signal(barrier, inc=1, device_id={axis: lax.rem(me + k, n)},
                            device_id_type=pl.DeviceIdType.MESH)

    pl.semaphore_wait(barrier, n - 1)

    @pl.loop(0, n // 4)
    def _(b):
        for j in range(4):
            k = b * 4 + j
            slot = j % 2
            u_copy(k, slot).wait()
            where = theirs[dest(k)]
            rows = lax.broadcasted_iota(jnp.int32, (CP, T), 0)
            pick = [(where[l:l + 1, :] == rows).astype(F32).astype(BF16) for l in range(el)]

            @pl.loop(0, D // NT)
            def _(i):
                cols = pl.ds(pl.multiple_of(i * NT, NT), NT)
                for l in range(el):
                    xin[l, j * CP:(j + 1) * CP, cols] = jnp.dot(
                        pick[l], ubuf[slot, :, cols], preferred_element_type=F32).astype(BF16)

            @pl.when(k + 2 < n)
            def _():
                u_copy(k + 2, slot).start()

        @pl.when(b == 0)
        def _():
            for cp in weights:
                cp.wait()

        for l in range(el):
            @pl.loop(0, FF // FT)
            def _(i):
                cols = pl.ds(pl.multiple_of(i * FT, FT), FT)
                h1 = jnp.dot(xin[l], v1[l, :, cols], preferred_element_type=F32)
                h3 = jnp.dot(xin[l], v3[l, :, cols], preferred_element_type=F32)
                z[l, :, cols] = (h1 * jax.nn.sigmoid(h1) * h3).astype(BF16)

        @pl.loop(0, D // NT)
        def _(i):
            cols = pl.ds(pl.multiple_of(i * NT, NT), NT)
            o0 = jnp.dot(z[0], v2[0, :, cols], preferred_element_type=F32)
            o1 = jnp.dot(z[1], v2[1, :, cols], preferred_element_type=F32)
            for j in range(4):
                both = jnp.concatenate([o0[j * CP:j * CP + C], o1[j * CP:j * CP + C]], axis=0)
                out[j, :, cols] = both.astype(BF16)

        for j in range(4):
            d = dest(b * 4 + j)

            @pl.when(d != me)
            def _():
                pltpu.make_async_copy(out.at[j], stage.at[d], o_sem.at[j]).start()

            @pl.when(d == me)
            def _():
                pltpu.make_async_copy(out.at[j], recv.at[me], o_sem.at[j]).start()

        for j in range(4):
            d = dest(b * 4 + j)

            @pl.when(d != me)
            def _():
                pltpu.make_async_copy(out.at[j], stage.at[d], o_sem.at[j]).wait()
                send(d).start()

            @pl.when(d == me)
            def _():
                pltpu.make_async_copy(out.at[j], recv.at[me], o_sem.at[j]).wait()

    y_copy.wait()

    @pl.loop(0, n // 4)
    def _(cc):
        for slot in range(2):
            c = cc * 2 + slot
            copies = []
            for i in range(2):
                e = _peer(n, me, c * 2 + i, False)

                @pl.when(e != me)
                def _():
                    pltpu.make_async_remote_copy(
                        src_ref=stage.at[e], dst_ref=recv.at[e],
                        send_sem=send_sem.at[e], recv_sem=recv_sem.at[e],
                        device_id={axis: me}, device_id_type=pl.DeviceIdType.MESH).wait_recv()
                copies.append(pltpu.make_async_copy(recv.at[e], rbuf.at[slot, i], r_sem.at[slot, i]))
                copies[i].start()

            @pl.when(c + 1 < n // 2)
            def _():
                m_copy(c + 1, 1 - slot).start()

            m_copy(c, slot).wait()
            lanes = lax.broadcasted_iota(jnp.int32, (T, KW), 1).astype(F32)
            for q in range(2 * el):
                sel[q] = (lanes == mbuf[slot, :, q:q + 1]).astype(F32).astype(BF16)
            for cp in copies:
                cp.wait()

            @pl.loop(0, D // NT)
            def _(i):
                cols = pl.ds(pl.multiple_of(i * NT, NT), NT)
                acc = y[:, cols]
                for q in range(2 * el):
                    at = (q % el) * (C2 - KW)
                    got = jnp.dot(sel[q], rbuf[slot, q // el, at:at + KW, cols], preferred_element_type=F32)
                    acc = acc + mbuf[slot, :, 2 * el + q:2 * el + q + 1] * got
                y[:, cols] = acc

    @pl.loop(0, D // NT)
    def _(i):
        cols = pl.ds(pl.multiple_of(i * NT, NT), NT)
        ubuf[0, :, cols] = y[:, cols].astype(BF16)

    done = pltpu.make_async_copy(ubuf.at[0], y_out, y_sem.at[0])
    done.start()
    done.wait()

    @pl.loop(0, n)
    def _(d):
        @pl.when(d != me)
        def _():
            send(d).wait_send()


def _window(C):
    return min(256, 2 * C)


def _run_exchange(n, axis, C, theirs, u_all, w1, w3, w2, marks, y0):
    T, D = y0.shape
    el, _, FF = w1.shape
    C2, CP = 2 * C, _up(C, 16)
    KW = _window(C)
    any_spec = pl.BlockSpec(memory_space=pl.ANY)
    dma = pltpu.SemaphoreType.DMA
    rows = n * 2 * C
    return pl.pallas_call(
        functools.partial(_exchange, n, axis),
        out_shape=(jax.ShapeDtypeStruct((T, D), BF16),
                   jax.ShapeDtypeStruct((n, C2, D), BF16),
                   jax.ShapeDtypeStruct((n, C2, D), BF16)),
        in_specs=[pl.BlockSpec(memory_space=pltpu.VMEM)] + [any_spec] * 6,
        out_specs=(any_spec,) * 3,
        scratch_shapes=[
            pltpu.VMEM((2, T, D), BF16),
            pltpu.VMEM((el, D, FF), BF16),
            pltpu.VMEM((el, D, FF), BF16),
            pltpu.VMEM((el, FF, D), BF16),
            pltpu.VMEM((el, 4 * CP, D), BF16),
            pltpu.VMEM((el, 4 * CP, FF), BF16),
            pltpu.VMEM((4, C2, D), BF16),
            pltpu.VMEM((T, D), F32),
            pltpu.VMEM((2, T, 4 * el), F32),
            pltpu.VMEM((2 * el, T, KW), BF16),
            pltpu.VMEM((2, 2, C2, D), BF16),
            dma((2,)), dma((3,)), dma((4,)), dma((1,)), dma((2,)), dma((2, 2)), dma((n,)), dma((n,)),
        ],
        compiler_params=pltpu.CompilerParams(
            collective_id=0, has_side_effects=True, vmem_limit_bytes=66 * 1000 * 1000),
        cost_estimate=pl.CostEstimate(
            flops=rows * 6 * D * FF + rows * 6 * T * D, bytes_accessed=rows * D * 8, transcendentals=rows * FF),
        name='exchange',
    )(theirs, u_all, w1, w3, w2, marks, y0)[0]


def solution(mesh):
    n = mesh.shape['expert']

    def local(x, idx, g, hot_tok, hot_g, ln1, wq, wk, wv, wo, ln2, w1, w3, w2):
        T, D = x.shape
        KC = idx.shape[1]
        el = w1.shape[0]
        E = el * n
        C = _capacity(T, KC, E)
        owner = HOT_ID // el
        lh = HOT_ID % el
        me = lax.axis_index('expert')

        own = me == owner
        hw = [lax.psum(jnp.where(own, w[lh], jnp.zeros((), BF16)), 'expert') for w in (w1, w3, w2)]

        same = idx[:, :, None] == jnp.arange(E, dtype=jnp.int32)
        has = jnp.any(same, axis=1)
        gate = jnp.sum(jnp.where(same, g[:, :, None], 0.0), axis=1)
        tri = jnp.tril(jnp.ones((T, T), BF16))
        upto = jnp.dot(tri, has.astype(BF16), preferred_element_type=F32)
        place = jnp.where(has, upto.astype(jnp.int32) - 1, -1)
        theirs = lax.all_to_all(place.T, 'expert', 0, 0, tiled=True).reshape(n, el, T)
        theirs = jnp.pad(theirs, ((0, 0), (0, 8 - el), (0, 0)), constant_values=-1)

        src = _peer(n, me, jnp.arange(n, dtype=jnp.int32), False)
        experts = (src[:, None] * el + jnp.arange(el, dtype=jnp.int32)).reshape(-1)
        shift = jnp.arange(E, dtype=jnp.int32) % el * (C - (2 * C - _window(C)))
        row = jnp.where(has, place + shift, -1).astype(F32)
        marks = jnp.stack([row.T[experts], gate.T[experts]]).reshape(2, n // 2, 2 * el, T)
        marks = marks.transpose(1, 3, 0, 2).reshape(n // 2, T, 4 * el)

        chunks = _attention_chunks(x, ln1, wq, wk, wv, wo, CHUNKS)
        u = _rms(chunks.send(None), ln2)
        u, *hw = lax.optimization_barrier((u, *hw))
        u_all = lax.all_gather(u, 'expert')

        hot_hit = hot_tok[:, None] == jnp.arange(T, dtype=jnp.int32)
        hot_rows = jnp.dot(hot_hit.astype(BF16), u, preferred_element_type=F32).astype(BF16)
        hot_out = _ffn(hot_rows, *hw)
        y0 = _gated([v[None, :] for v in _parts(hot_g)], hot_hit.T, hot_out)
        return _run_exchange(n, 'expert', C, theirs, u_all, w1, w3, w2, marks, y0)

    tk = ('data', 'expert')
    rep3 = P(None, None, None)
    exp3 = P('expert', None, None)
    return jax.shard_map(
        local, mesh=mesh,
        in_specs=(P(tk, None), P(tk, None), P(tk, None), P(tk), P(tk), P(None),
                  rep3, rep3, rep3, rep3, P(None), exp3, exp3, exp3),
        out_specs=P(tk, None), check_vma=False)
```

```python
import functools
import math

import jax
import jax.numpy as jnp
from jax import lax
from jax.experimental import pallas as pl
from jax.experimental.pallas import tpu as pltpu
from jax.sharding import PartitionSpec as P

EPS = 1e-6
ROPE_BASE = 10000.0
HOT_ID = 1
CHUNKS = 1
F32 = jnp.float32
BF16 = jnp.bfloat16


def _rms(v, w):
    v = v.astype(F32)
    return (v * lax.rsqrt(jnp.mean(v * v, axis=-1, keepdims=True) + EPS) * w).astype(BF16)


def _rope(t, start):
    n_tok, _, dh = t.shape
    half = dh // 2
    freq = ROPE_BASE ** (-jnp.arange(half, dtype=F32) / half)
    ang = (start + jnp.arange(n_tok, dtype=F32))[:, None] * freq[None, :]
    cos = jnp.cos(ang)[:, None, :]
    sin = jnp.sin(ang)[:, None, :]
    t1, t2 = t[..., :half], t[..., half:]
    return jnp.concatenate([t1 * cos - t2 * sin, t2 * cos + t1 * sin], axis=-1)


def _attention_chunks(x, ln1, wq, wk, wv, wo, chunks):
    n_tok = x.shape[0]
    dh = wq.shape[2]
    step = n_tok // chunks
    ks, vs = [], []
    before = None
    for c in range(chunks):
        lo = c * step
        xc = x[lo:lo + step]
        if before is not None:
            xc, _ = lax.optimization_barrier((xc, before))
        a = _rms(xc, ln1)
        q = _rope(jnp.einsum('td,dhk->thk', a, wq, preferred_element_type=F32), lo).astype(BF16)
        ks.append(_rope(jnp.einsum('td,dhk->thk', a, wk, preferred_element_type=F32), lo).astype(BF16))
        vs.append(jnp.einsum('td,dhk->thk', a, wv, preferred_element_type=F32).astype(BF16))
        k = jnp.concatenate(ks, axis=0)
        v = jnp.concatenate(vs, axis=0)
        s = jnp.einsum('qhk,shk->hqs', q, k, preferred_element_type=F32) * dh ** -0.5
        mask = (lo + jnp.arange(step))[:, None] >= jnp.arange(lo + step)[None, :]
        p = jax.nn.softmax(jnp.where(mask[None], s, -jnp.inf), axis=-1).astype(BF16)
        o = jnp.einsum('hqs,shk->qhk', p, v, preferred_element_type=F32).astype(BF16)
        out = jnp.einsum('qhk,hkd->qd', o, wo, preferred_element_type=F32)
        before = yield (xc.astype(F32) + out).astype(BF16)


def _capacity(t, kc, n_exp):
    c0 = (t * kc + n_exp - 2) // (n_exp - 1)
    return 8 * ((3 * c0 + 15) // 16)


def _ffn(a, w1, w3, w2):
    h1 = jnp.dot(a, w1, preferred_element_type=F32)
    h3 = jnp.dot(a, w3, preferred_element_type=F32)
    z = (jax.nn.silu(h1) * h3).astype(BF16)
    return jnp.dot(z, w2, preferred_element_type=F32).astype(BF16)


def _up(v, m):
    return (v + m - 1) // m * m


ORDER4 = (4, 14, 28, 13, 12, 20, 1, 19, 3, 8, 24, 16, 17, 2, 21, 5,
          29, 15, 31, 9, 23, 7, 0, 18, 25, 27, 11, 6, 10, 22, 26, 30)


def _side(n):
    return math.isqrt(n // 2)


def _offset(n, k):
    side = _side(n)
    order = ORDER4 if side == 4 else tuple(i % side + i // side % side * 4 + i // (n // 2) * 16 for i in range(n))
    bit0, bit1 = lax.rem(lax.div(k, 8), 2), lax.div(k, 16)
    q = lax.rem(k, 8)
    power = (1 + 3 * lax.rem(q, 2)) * (1 + 15 * lax.rem(lax.div(q, 2), 2)) * (1 + 255 * lax.div(q, 4))

    def digit(vals):
        a, b, c, d = (sum(v * 4 ** i for i, v in enumerate(vals[h * 8:h * 8 + 8])) for h in range(4))
        pack = (a * (1 - bit0) + b * bit0) * (1 - bit1) + (c * (1 - bit0) + d * bit0) * bit1
        return lax.rem(lax.div(pack, power), 4)

    return digit([v % 4 for v in order]), digit([v // 4 % 4 for v in order]), digit([v // 16 for v in order])


def _peer(n, me, k, sending):
    side = _side(n)
    core, chip = lax.rem(me, 2), lax.div(me, 2)
    dx, dy, other = _offset(n, k)
    their = lax.rem(core + other, 2)
    sign = 1 - 2 * core if sending else 2 * their - 1
    px = lax.rem(lax.rem(chip, side) + sign * dx + side, side)
    py = lax.rem(lax.div(chip, side) + sign * dy + side, side)
    return (py * side + px) * 2 + their


def _exchange(n, axis, theirs, u_all, w1, w3, w2, marks, y0,
              y_out, recv, stage,
              ubuf, v1, v3, v2, xin, z, out, y, mbuf, sel, rbuf,
              u_sem, w_sem, o_sem, y_sem, m_sem, r_sem, send_sem, recv_sem):
    T, D = y.shape
    el, CP = 2, xin.shape[1] // 4
    C2 = recv.shape[1]
    C = C2 // 2
    FF = z.shape[2]
    KW = sel.shape[2]
    FT, NT = min(256, FF), min(256, D)
    me = lax.axis_index(axis)

    def dest(k):
        return _peer(n, me, k, True)

    def u_copy(k, slot):
        return pltpu.make_async_copy(u_all.at[dest(k)], ubuf.at[slot], u_sem.at[slot])

    def m_copy(c, slot):
        return pltpu.make_async_copy(marks.at[c], mbuf.at[slot], m_sem.at[slot])

    def send(d):
        return pltpu.make_async_remote_copy(
            src_ref=stage.at[d], dst_ref=recv.at[me],
            send_sem=send_sem.at[d], recv_sem=recv_sem.at[me],
            device_id={axis: d}, device_id_type=pl.DeviceIdType.MESH)

    weights = [pltpu.make_async_copy(a, b, w_sem.at[i])
               for i, (a, b) in enumerate(((w1, v1), (w3, v3), (w2, v2)))]
    u_copy(0, 0).start()
    u_copy(1, 1).start()
    for cp in weights:
        cp.start()
    y_copy = pltpu.make_async_copy(y0, y, y_sem.at[0])
    y_copy.start()
    m_copy(0, 0).start()

    barrier = pltpu.get_barrier_semaphore()

    @pl.loop(1, n)
    def _(k):
        pl.semaphore_signal(barrier, inc=1, device_id={axis: lax.rem(me + k, n)},
                            device_id_type=pl.DeviceIdType.MESH)

    pl.semaphore_wait(barrier, n - 1)

    def step(first, batch):
        m = batch * CP
        for j in range(batch):
            k = first + j
            slot = j % 2
            u_copy(k, slot).wait()
            where = theirs[dest(k)]
            rows = lax.broadcasted_iota(jnp.int32, (CP, T), 0)
            pick = [(where[l:l + 1, :] == rows).astype(F32).astype(BF16) for l in range(el)]

            @pl.loop(0, D // NT)
            def _(i):
                cols = pl.ds(pl.multiple_of(i * NT, NT), NT)
                for l in range(el):
                    xin[l, j * CP:(j + 1) * CP, cols] = jnp.dot(
                        pick[l], ubuf[slot, :, cols], preferred_element_type=F32).astype(BF16)

            @pl.when(k + 2 < n)
            def _():
                u_copy(k + 2, slot).start()

        @pl.when(first == 0)
        def _():
            for cp in weights:
                cp.wait()

        for l in range(el):
            @pl.loop(0, FF // FT)
            def _(i):
                cols = pl.ds(pl.multiple_of(i * FT, FT), FT)
                h1 = jnp.dot(xin[l, :m], v1[l, :, cols], preferred_element_type=F32)
                h3 = jnp.dot(xin[l, :m], v3[l, :, cols], preferred_element_type=F32)
                z[l, :m, cols] = (h1 * jax.nn.sigmoid(h1) * h3).astype(BF16)

        @pl.loop(0, D // NT)
        def _(i):
            cols = pl.ds(pl.multiple_of(i * NT, NT), NT)
            o0 = jnp.dot(z[0, :m], v2[0, :, cols], preferred_element_type=F32)
            o1 = jnp.dot(z[1, :m], v2[1, :, cols], preferred_element_type=F32)
            for j in range(batch):
                both = jnp.concatenate([o0[j * CP:j * CP + C], o1[j * CP:j * CP + C]], axis=0)
                out[j, :, cols] = both.astype(BF16)

        for j in range(batch):
            d = dest(first + j)

            @pl.when(d != me)
            def _():
                pltpu.make_async_copy(out.at[j], stage.at[d], o_sem.at[j]).start()

            @pl.when(d == me)
            def _():
                pltpu.make_async_copy(out.at[j], recv.at[me], o_sem.at[j]).start()

        for j in range(batch):
            d = dest(first + j)

            @pl.when(d != me)
            def _():
                pltpu.make_async_copy(out.at[j], stage.at[d], o_sem.at[j]).wait()
                send(d).start()

            @pl.when(d == me)
            def _():
                pltpu.make_async_copy(out.at[j], recv.at[me], o_sem.at[j]).wait()

    @pl.loop(0, 2)
    def _(b):
        step(b * 2, 2)

    @pl.loop(1, n // 4)
    def _(b):
        step(b * 4, 4)

    y_copy.wait()

    @pl.loop(0, n // 4)
    def _(cc):
        for slot in range(2):
            c = cc * 2 + slot
            copies = []
            for i in range(2):
                e = _peer(n, me, c * 2 + i, False)

                @pl.when(e != me)
                def _():
                    pltpu.make_async_remote_copy(
                        src_ref=stage.at[e], dst_ref=recv.at[e],
                        send_sem=send_sem.at[e], recv_sem=recv_sem.at[e],
                        device_id={axis: me}, device_id_type=pl.DeviceIdType.MESH).wait_recv()
                copies.append(pltpu.make_async_copy(recv.at[e], rbuf.at[slot, i], r_sem.at[slot, i]))
                copies[i].start()

            @pl.when(c + 1 < n // 2)
            def _():
                m_copy(c + 1, 1 - slot).start()

            m_copy(c, slot).wait()
            lanes = lax.broadcasted_iota(jnp.int32, (T, KW), 1).astype(F32)
            for q in range(2 * el):
                sel[q] = (lanes == mbuf[slot, :, q:q + 1]).astype(F32).astype(BF16)
            for cp in copies:
                cp.wait()

            @pl.loop(0, D // NT)
            def _(i):
                cols = pl.ds(pl.multiple_of(i * NT, NT), NT)
                acc = y[:, cols]
                for q in range(2 * el):
                    at = (q % el) * (C2 - KW)
                    got = jnp.dot(sel[q], rbuf[slot, q // el, at:at + KW, cols], preferred_element_type=F32)
                    acc = acc + mbuf[slot, :, 2 * el + q:2 * el + q + 1] * got
                y[:, cols] = acc

    @pl.loop(0, D // NT)
    def _(i):
        cols = pl.ds(pl.multiple_of(i * NT, NT), NT)
        ubuf[0, :, cols] = y[:, cols].astype(BF16)

    done = pltpu.make_async_copy(ubuf.at[0], y_out, y_sem.at[0])
    done.start()
    done.wait()

    @pl.loop(0, n)
    def _(d):
        @pl.when(d != me)
        def _():
            send(d).wait_send()


def _window(C):
    return min(256, 2 * C)


def _run_exchange(n, axis, C, theirs, u_all, w1, w3, w2, marks, y0):
    T, D = y0.shape
    el, _, FF = w1.shape
    C2, CP = 2 * C, _up(C, 16)
    KW = _window(C)
    any_spec = pl.BlockSpec(memory_space=pl.ANY)
    dma = pltpu.SemaphoreType.DMA
    rows = n * 2 * C
    return pl.pallas_call(
        functools.partial(_exchange, n, axis),
        out_shape=(jax.ShapeDtypeStruct((T, D), BF16),
                   jax.ShapeDtypeStruct((n, C2, D), BF16),
                   jax.ShapeDtypeStruct((n, C2, D), BF16)),
        in_specs=[pl.BlockSpec(memory_space=pltpu.VMEM)] + [any_spec] * 6,
        out_specs=(any_spec,) * 3,
        scratch_shapes=[
            pltpu.VMEM((2, T, D), BF16),
            pltpu.VMEM((el, D, FF), BF16),
            pltpu.VMEM((el, D, FF), BF16),
            pltpu.VMEM((el, FF, D), BF16),
            pltpu.VMEM((el, 4 * CP, D), BF16),
            pltpu.VMEM((el, 4 * CP, FF), BF16),
            pltpu.VMEM((4, C2, D), BF16),
            pltpu.VMEM((T, D), F32),
            pltpu.VMEM((2, T, 4 * el), F32),
            pltpu.VMEM((2 * el, T, KW), BF16),
            pltpu.VMEM((2, 2, C2, D), BF16),
            dma((2,)), dma((3,)), dma((4,)), dma((1,)), dma((2,)), dma((2, 2)), dma((n,)), dma((n,)),
        ],
        compiler_params=pltpu.CompilerParams(
            collective_id=0, has_side_effects=True, vmem_limit_bytes=66 * 1000 * 1000),
        cost_estimate=pl.CostEstimate(
            flops=rows * 6 * D * FF + rows * 6 * T * D, bytes_accessed=rows * D * 8, transcendentals=rows * FF),
        name='exchange',
    )(theirs, u_all, w1, w3, w2, marks, y0)[0]


def solution(mesh):
    n = mesh.shape['expert']

    def local(x, idx, g, hot_tok, hot_g, ln1, wq, wk, wv, wo, ln2, w1, w3, w2):
        T, D = x.shape
        KC = idx.shape[1]
        el = w1.shape[0]
        E = el * n
        C = _capacity(T, KC, E)
        owner = HOT_ID // el
        lh = HOT_ID % el
        me = lax.axis_index('expert')

        own = me == owner
        hw = [lax.psum(jnp.where(own, w[lh], jnp.zeros((), BF16)), 'expert') for w in (w1, w3, w2)]

        same = idx[:, :, None] == jnp.arange(E, dtype=jnp.int32)
        has = jnp.any(same, axis=1)
        gate = jnp.sum(jnp.where(same, g[:, :, None], 0.0), axis=1)
        tri = jnp.tril(jnp.ones((T, T), BF16))
        upto = jnp.dot(tri, has.astype(BF16), preferred_element_type=F32)
        place = jnp.where(has, upto.astype(jnp.int32) - 1, -1)
        theirs = lax.all_to_all(place.T, 'expert', 0, 0, tiled=True).reshape(n, el, T)
        theirs = jnp.pad(theirs, ((0, 0), (0, 8 - el), (0, 0)), constant_values=-1)

        src = _peer(n, me, jnp.arange(n, dtype=jnp.int32), False)
        experts = (src[:, None] * el + jnp.arange(el, dtype=jnp.int32)).reshape(-1)
        shift = jnp.arange(E, dtype=jnp.int32) % el * (C - (2 * C - _window(C)))
        row = jnp.where(has, place + shift, -1).astype(F32)
        marks = jnp.stack([row.T[experts], gate.T[experts]]).reshape(2, n // 2, 2 * el, T)
        marks = marks.transpose(1, 3, 0, 2).reshape(n // 2, T, 4 * el)

        chunks = _attention_chunks(x, ln1, wq, wk, wv, wo, CHUNKS)
        u = _rms(chunks.send(None), ln2)
        u, *hw = lax.optimization_barrier((u, *hw))
        u_all = lax.all_gather(u, 'expert')

        hot_hit = hot_tok[:, None] == jnp.arange(T, dtype=jnp.int32)
        hot_rows = jnp.dot(hot_hit.astype(BF16), u, preferred_element_type=F32).astype(BF16)
        hot_out = _ffn(hot_rows, *hw)
        token_g = jnp.sum(jnp.where(hot_hit, hot_g[:, None], 0.0), axis=0)
        y0 = token_g[:, None] * jnp.dot(hot_hit.T.astype(BF16), hot_out, preferred_element_type=F32)
        return _run_exchange(n, 'expert', C, theirs, u_all, w1, w3, w2, marks, y0)

    tk = ('data', 'expert')
    rep3 = P(None, None, None)
    exp3 = P('expert', None, None)
    return jax.shard_map(
        local, mesh=mesh,
        in_specs=(P(tk, None), P(tk, None), P(tk, None), P(tk), P(tk), P(None),
                  rep3, rep3, rep3, rep3, P(None), exp3, exp3, exp3),
        out_specs=P(tk, None), check_vma=False)
```
